32 devices in a mesh: dp: 2 (over x), expert: 16 (over z, y, core).
Axes of the slice: x: 2, y: 2, z: 4, core: 2. Of those that a mesh axis runs over, the one named last changes fastest.
Arguments:
- tokens: bfloat16 [4096, 1024], P(('dp', 'expert')), may hold values from -6 to 6
- out_grad: bfloat16 [4096, 1024], P(('dp', 'expert')), may hold values from -6 to 6
- expert_ids: int32 [4096, 3], P(('dp', 'expert')), may hold values from 0 to 15, all different within a row; in each aligned block of 128 rows (0 to 127, 128 to 255, ...) at most 30 rows name the same one
- gate_probs: float32 [4096, 3], P(('dp', 'expert')), may hold values from 0.1 to 0.6
- saved_pre: bfloat16 [2, 16, 480, 1536], P('dp', 'expert'), may hold values from -6 to 6
- gate_weight: bfloat16 [16, 1024, 768], P('expert', 'dp'), may hold values from -0.1875 to 0.1875
- up_weight: bfloat16 [16, 1024, 768], P('expert', 'dp'), may hold values from -0.1875 to 0.1875
- down_weight: bfloat16 [16, 1024, 768], P('expert', 'dp'), may hold values from -0.21875 to 0.21875
- basis: bfloat16 [16, 1024, 256], P('expert', 'dp'), may hold values from -0.1875 to 0.1875
Outputs:
- in_grad: bfloat16 [4096, 1024], P(('dp', 'expert'))
- proj_grads: float32 [16, 3, 256, 768], P('expert', None, 'dp')
The draws below stay inside these ranges and needn't reach their ends.
Inputs may be any that keep to these rules, and one draw needn't show every extreme that they name: `expert_ids`: each token names 3 different experts. The rows of one device name one expert at most 30 times, and on some devices some expert exactly 30 times.
All inputs are finite; a program needn't handle non-finite values.
Results may differ from the reference program's by a relative error of at most 0.0091.
Values may be sent and summed in bfloat16 or wider, within the bound.
A program may use at most 64 MiB of HBM per device.

```python
import math
import jax
import jax.numpy as jnp
import numpy as np
from jax import lax

D = 1024
FF = 768
RANK = 256
TOPK = 3
TOK_DEV = 128
EXPERTS = 16
CAP = 30
SLOTS = 480
TOKENS = 4096
N_DP = 2
N_EXPERT = 16


def block_scale(stream_key, extent, cuts, smallest, largest):
    loudness, own = 1.0, jax.random.fold_in(stream_key, 6)
    for dim, blocks in cuts:
        draws = jnp.exp(jax.random.uniform(jax.random.fold_in(own, dim), (blocks,), jnp.float32, smallest / len(cuts), largest / len(cuts)))
        loudness = loudness * jnp.repeat(draws, extent[dim] // blocks).reshape([-1 if axis == dim else 1 for axis in range(len(extent))])
    return loudness


def assign_block(own_key, own, number, rows, amount, top, reach, slope):
    order = jax.random.permutation(own_key, amount)
    packed, ordinary = load_shares(amount, rows * top, reach, slope, True), load_shares(amount, rows * top, reach, slope, False)
    places = jnp.arange(amount)

    def named(sizes, rotation):
        used = int((sizes > 0).sum())
        fixed = max(1, used // 4)
        moved = fixed + (places - fixed + rotation * (used - fixed)) % max(1, amount - fixed)
        return jnp.zeros((amount,), jnp.int32).at[order[jnp.where(places < fixed, places, moved)]].set(jnp.asarray(sizes, jnp.int32))

    sizes = jnp.where(number % 4 == 0, named(packed, number // 4), named(ordinary, number - number // 4 - 1))
    mixed = jax.random.permutation(jax.random.fold_in(own, 3), amount)
    source_of, sink = mixed[0:amount // 2 * 2:2], mixed[1:amount // 2 * 2:2]
    margin = jnp.minimum(sizes[source_of] - 1, reach - sizes[sink]) // 2
    margin = jnp.where((source_of == order[0]) | (sink == order[0]) | (sizes[sink] == 0), 0, jnp.maximum(margin, 0))
    moved = jax.random.randint(jax.random.fold_in(own, 4), (amount // 2,), 0, 1 << 20) % (margin + 1)
    sizes = sizes.at[source_of].add(-moved).at[sink].add(moved)
    members = jnp.searchsorted(jnp.cumsum(sizes), jnp.arange(rows * top), side="right").astype(jnp.int32)
    grid = members.reshape(top, rows).T
    grid = grid[jax.random.permutation(jax.random.fold_in(own, 1), rows)]
    rotation = jax.random.randint(jax.random.fold_in(own, 2), (rows, 1), 0, top)
    return jnp.take_along_axis(grid, (jnp.arange(top)[None, :] + rotation) % top, axis=1)


def load_shares(count, total, limit, skew, full):
    portions = [(1 << 20) // math.isqrt(grade ** skew) + 1 for grade in range(1, count + 1)]
    largest = limit if full else min(limit, max(-(-total // count), total * portions[0] // sum(portions)))
    least = 1 if total - largest >= count - 1 else 0
    counts, surplus = [largest] + [least] * (count - 1), total - largest - least * (count - 1)
    while surplus > 0:
        candidates = [i for i in range(1, count) if counts[i] < largest] or [i for i in range(1, count) if counts[i] < limit]
        mass, budget = sum([portions[i] for i in candidates]), surplus
        for i in candidates:
            addition = min(limit - counts[i], max(1, budget * portions[i] // mass), surplus)
            counts[i] = counts[i] + addition
            surplus = surplus - addition
    return np.array(counts)


def scatter_about(rng, dims, width, reach, shards=(), kind=jnp.bfloat16):
    entries = width * jax.random.normal(rng, dims, jnp.float32)
    if shards:
        entries = entries * block_scale(rng, dims, shards, -0.22, 0.18)
    return jnp.clip(entries, -reach, reach).astype(kind)


def setup_inputs(seed: int = 0) -> dict:
    arg_keys = jax.random.split(jax.random.key(seed), 10)
    tokens = scatter_about(arg_keys[0], (TOKENS, D), 1.0, 6.0, ((0, 32),))
    out_grad = scatter_about(arg_keys[1], (TOKENS, D), 1.0, 6.0, ((0, 32),))
    expert_ids_keys = jax.random.split(jax.random.fold_in(arg_keys[2], 1), TOKENS // TOK_DEV)
    expert_ids_turns = jax.random.permutation(jax.random.fold_in(arg_keys[2], 3), TOKENS // TOK_DEV)
    expert_ids = jax.vmap(lambda own, number: assign_block(jax.random.fold_in(arg_keys[2], 2), own, number, TOK_DEV, EXPERTS, TOPK, CAP, 2))(expert_ids_keys, expert_ids_turns).reshape((TOKENS, TOPK))
    gate_probs = jnp.clip(0.1 + 0.5 * jax.random.uniform(arg_keys[3], (TOKENS, TOPK), jnp.float32) ** block_scale(arg_keys[3], (TOKENS, TOPK), ((0, 32),), -0.2, 0.2), 0.1, 0.6)
    saved_pre = scatter_about(arg_keys[4], (N_DP, EXPERTS, SLOTS, 2 * FF), 1.5, 6.0, ((0, 2), (1, 16)))
    gate_weight = scatter_about(arg_keys[5], (EXPERTS, D, FF), D ** -0.5, 0.1875, ((0, 16), (1, 2)))
    up_weight = scatter_about(arg_keys[6], (EXPERTS, D, FF), D ** -0.5, 0.1875, ((0, 16), (1, 2)))
    down_weight = scatter_about(arg_keys[7], (EXPERTS, D, FF), FF ** -0.5, 0.21875, ((0, 16), (1, 2)))
    basis = scatter_about(arg_keys[8], (EXPERTS, D, RANK), D ** -0.5, 0.1875, ((0, 16), (1, 2)))
    return {"tokens": tokens, "out_grad": out_grad, "expert_ids": expert_ids, "gate_probs": gate_probs, "saved_pre": saved_pre, "gate_weight": gate_weight, "up_weight": up_weight, "down_weight": down_weight, "basis": basis}


def slot_tables(expert_ids):
    devices = N_DP * N_EXPERT
    ids = expert_ids.reshape(devices, TOK_DEV, TOPK)
    onehot = (ids[:, :, :, None] == jnp.arange(EXPERTS, dtype=jnp.int32)[None, None, None, :]).astype(jnp.int32)
    per_token = jnp.sum(onehot, axis=2)
    before = jnp.cumsum(per_token, axis=1) - per_token
    position = jnp.sum(onehot * before[:, :, None, :], axis=3)
    device = jnp.arange(devices, dtype=jnp.int32)[:, None, None]
    group = device // N_EXPERT
    source = device % N_EXPERT
    flat = (group * EXPERTS + ids) * SLOTS + source * CAP + position
    token_index = device * TOK_DEV + jnp.arange(TOK_DEV, dtype=jnp.int32)[None, :, None]
    token_index = jnp.broadcast_to(token_index, ids.shape)
    choice_index = jnp.broadcast_to(jnp.arange(TOPK, dtype=jnp.int32)[None, None, :], ids.shape)
    table_token = jnp.full((N_DP * EXPERTS * SLOTS,), -1, jnp.int32).at[flat.reshape(-1)].set(token_index.reshape(-1))
    table_choice = jnp.zeros((N_DP * EXPERTS * SLOTS,), jnp.int32).at[flat.reshape(-1)].set(choice_index.reshape(-1))
    return table_token.reshape(N_DP, EXPERTS, SLOTS), table_choice.reshape(N_DP, EXPERTS, SLOTS)


def reference(tokens, out_grad, expert_ids, gate_probs, saved_pre, gate_weight, up_weight, down_weight, basis):
    table_token, table_choice = slot_tables(expert_ids)

    def per_expert(accum, expert):
        w_gate = gate_weight[expert]
        w_up = up_weight[expert]
        w_down = down_weight[expert]
        w_basis = basis[expert]

        def per_group(carry, group):
            total, projected = carry
            taken = table_token[group, expert]
            chosen = table_choice[group, expert]
            filled = taken >= 0
            picked = jnp.maximum(taken, 0).astype(jnp.int32)
            x_rows = jnp.where(filled[:, None], tokens[picked], jnp.zeros((), jnp.bfloat16))
            weight_pick = gate_probs[picked, chosen]
            scaled = (out_grad[picked].astype(jnp.float32) * weight_pick[:, None]).astype(jnp.bfloat16)
            dy_rows = jnp.where(filled[:, None], scaled, jnp.zeros((), jnp.bfloat16))
            pre = saved_pre[group, expert].astype(jnp.float32)
            gate_pre = pre[:, :FF]
            up_pre = pre[:, FF:]
            hidden_grad = jnp.dot(dy_rows, w_down, preferred_element_type=jnp.float32)
            x_proj = jnp.dot(x_rows, w_basis, preferred_element_type=jnp.float32).astype(jnp.bfloat16)
            dy_proj = jnp.dot(dy_rows, w_basis, preferred_element_type=jnp.float32).astype(jnp.bfloat16)
            sig = jax.nn.sigmoid(gate_pre)
            hid = (gate_pre * sig * up_pre).astype(jnp.bfloat16)
            up_grad = (hidden_grad * gate_pre * sig).astype(jnp.bfloat16)
            gate_grad = (hidden_grad * up_pre * sig * (1.0 + gate_pre * (1.0 - sig))).astype(jnp.bfloat16)
            terms = jnp.stack([
                jnp.dot(x_proj.T, gate_grad, preferred_element_type=jnp.float32),
                jnp.dot(x_proj.T, up_grad, preferred_element_type=jnp.float32),
                jnp.dot(dy_proj.T, hid, preferred_element_type=jnp.float32)])
            row_grad = jnp.dot(gate_grad, w_gate.T, preferred_element_type=jnp.float32)
            row_grad = row_grad + jnp.dot(up_grad, w_up.T, preferred_element_type=jnp.float32)
            row_grad = row_grad.astype(jnp.bfloat16).astype(jnp.float32)
            row_grad = jnp.where(filled[:, None], row_grad, jnp.zeros((), jnp.float32))
            total = total.at[picked].add(row_grad)
            return (total, projected + terms), None

        start = (accum, jnp.zeros((3, RANK, FF), jnp.float32))
        (accum, projected), unused = lax.scan(per_group, start, jnp.arange(N_DP, dtype=jnp.int32))
        return accum, projected

    accum = jnp.zeros((TOKENS, D), jnp.float32)
    accum, proj_grads = lax.scan(per_expert, accum, jnp.arange(EXPERTS, dtype=jnp.int32))
    return accum.astype(jnp.bfloat16), proj_grads
```

```python
import functools
import jax
import jax.numpy as jnp
from jax import lax
from jax.experimental import pallas as pl
from jax.experimental.pallas import tpu as pltpu
from jax.sharding import PartitionSpec as P

MESH = pl.DeviceIdType.MESH
F32 = jnp.float32
BF16 = jnp.bfloat16


def dot(left, right, dims):
    return lax.dot_general(left, right, (dims, ((), ())), preferred_element_type=F32)


NN = ((1,), (0,))
TN = ((0,), (0,))
NT = ((1,), (1,))


def kernel(
    n_dp, n_ex, cap, cp, cw,
    ids, probs, tok, og, pre_h, gw, uw, dw, bs,
    in_ref, proj_ref,
    sx, sg, rx, rg, dfull, bfull, gfull, ufull, pre, act_a, act_b, hid, ggrad, ugrad,
    rs, rr, terms, psend, prec,
    local_sem, dy_s, dy_r, x_s, x_r, down_s, down_r, base_s, base_r,
    gate_s, gate_r, up_s, up_r, ret_s, ret_r, proj_s, proj_r,
):
    my_dp = lax.axis_index("dp")
    me = lax.axis_index("expert")
    rows = n_ex * cp
    tokens, width = tok.shape
    topk = ids.shape[1]
    slots, hidden2 = pre.shape
    hidden = hidden2 // 2
    part = width // n_dp
    nc = part // cw
    rank = bfull.shape[1]
    rk = rank // n_dp
    shift = cp.bit_length() - 1

    def block(owner):
        return pl.ds(pl.multiple_of(owner * cp, cp), cp)

    def wpart(owner):
        return pl.ds(pl.multiple_of(owner * part, part), part)

    def ex_peer(k):
        return lax.rem(me + k, n_ex)

    def ex_from(k):
        return lax.rem(me + n_ex - k, n_ex)

    def dp_peer(i):
        return lax.rem(my_dp + i, n_dp)

    def dp_from(i):
        return lax.rem(my_dp + n_dp - i, n_dp)

    barrier = pltpu.get_barrier_semaphore()

    @pl.loop(1, n_ex)
    def _(k):
        pl.semaphore_signal(barrier, inc=1, device_id={"expert": ex_peer(k)}, device_id_type=MESH)

    for i in range(1, n_dp):
        pl.semaphore_signal(barrier, inc=1, device_id={"dp": dp_peer(i)}, device_id_type=MESH)

    local = [
        pltpu.make_async_copy(pre_h.at[0, 0], pre, local_sem.at[0]),
        pltpu.make_async_copy(dw.at[0], dfull.at[wpart(my_dp)], local_sem.at[1]),
        pltpu.make_async_copy(bs.at[0], bfull.at[wpart(my_dp)], local_sem.at[2]),
    ]
    for c in range(nc):
        src = pl.ds(c * cw, cw)
        local.append(
            pltpu.make_async_copy(gw.at[0, src], gfull.at[my_dp * nc + c], local_sem.at[3 + 2 * c])
        )
        local.append(
            pltpu.make_async_copy(uw.at[0, src], ufull.at[my_dp * nc + c], local_sem.at[4 + 2 * c])
        )
    for copy in local:
        copy.start()

    lane = lax.broadcasted_iota(jnp.int32, (tokens, rows), 1)
    lane_expert = lax.shift_right_logical(lane, shift)
    lane_slot = lax.bitwise_and(lane, cp - 1)
    names = [ids[:, k : k + 1] == lane_expert for k in range(topk)]
    any_name = functools.reduce(jnp.logical_or, names)
    one, zero = jnp.ones((), F32), jnp.zeros((), F32)
    named = jnp.where(any_name, one, zero).astype(BF16)
    below = lax.broadcasted_iota(jnp.int32, (tokens, tokens), 0) > lax.broadcasted_iota(
        jnp.int32, (tokens, tokens), 1
    )
    before = dot(jnp.where(below, one, zero).astype(BF16), named, NN)
    at_slot = before == lane_slot.astype(F32)
    picks = [
        jnp.where(jnp.logical_and(name, at_slot), one, zero).astype(BF16) for name in names
    ]
    pick = jnp.where(jnp.logical_and(any_name, at_slot), one, zero).astype(BF16)
    grads = [
        (og[...].astype(F32) * probs[:, k : k + 1]).astype(BF16) for k in range(topk)
    ]
    sg[...] = dot(jnp.concatenate(picks, axis=0), jnp.concatenate(grads, axis=0), TN).astype(BF16)

    pl.semaphore_wait(barrier, n_ex - 1 + n_dp - 1)

    def down_copy(i, owner, peer):
        return pltpu.make_async_remote_copy(
            dw.at[0], dfull.at[wpart(owner)], down_s.at[i], down_r.at[i],
            device_id={"dp": peer}, device_id_type=MESH,
        )

    def base_copy(i, owner, peer):
        return pltpu.make_async_remote_copy(
            bs.at[0], bfull.at[wpart(owner)], base_s.at[i], base_r.at[i],
            device_id={"dp": peer}, device_id_type=MESH,
        )

    def gate_copy(i, c, owner, peer):
        return pltpu.make_async_remote_copy(
            gw.at[0, pl.ds(c * cw, cw)], gfull.at[owner * nc + c], gate_s.at[i, c], gate_r.at[i, c],
            device_id={"dp": peer}, device_id_type=MESH,
        )

    def up_copy(i, c, owner, peer):
        return pltpu.make_async_remote_copy(
            uw.at[0, pl.ds(c * cw, cw)], ufull.at[owner * nc + c], up_s.at[i, c], up_r.at[i, c],
            device_id={"dp": peer}, device_id_type=MESH,
        )

    def row_copy(src, dst, send, recv, k, peer, owner):
        return pltpu.make_async_remote_copy(
            src.at[block(peer)], dst.at[block(owner)], send.at[k], recv.at[k],
            device_id={"expert": peer}, device_id_type=MESH,
        )

    def ret_copy(n, j, k, peer, owner):
        return pltpu.make_async_remote_copy(
            rs.at[j, block(peer)], rr.at[j, block(owner)], ret_s.at[n, k], ret_r.at[n, k],
            device_id={"expert": peer}, device_id_type=MESH,
        )

    def proj_copy(i, peer):
        return pltpu.make_async_remote_copy(
            psend.at[i], prec.at[i], proj_s.at[i], proj_r.at[i],
            device_id={"dp": peer}, device_id_type=MESH,
        )

    for i in range(1, n_dp):
        down_copy(i, my_dp, dp_peer(i)).start()

    @pl.loop(1, n_ex)
    def _(k):
        row_copy(sg, rg, dy_s, dy_r, k, ex_peer(k), me).start()

    for i in range(1, n_dp):
        base_copy(i, my_dp, dp_peer(i)).start()
    for i in range(1, n_dp):
        for c in range(nc):
            gate_copy(i, c, my_dp, dp_peer(i)).start()
            up_copy(i, c, my_dp, dp_peer(i)).start()

    sx[...] = dot(pick, tok[...], TN).astype(BF16)

    @pl.loop(1, n_ex)
    def _(k):
        row_copy(sx, rx, x_s, x_r, k, ex_peer(k), me).start()

    rg[block(me), :] = sg[block(me), :]
    rx[block(me), :] = sx[block(me), :]

    local[0].wait()
    row = lax.broadcasted_iota(jnp.int32, (rows, slots), 0)
    inner = lax.bitwise_and(row, cp - 1)
    source = lax.shift_right_logical(row, shift) * cap + inner
    spread_mask = jnp.logical_and(
        source == lax.broadcasted_iota(jnp.int32, (rows, slots), 1), inner < cap
    )
    spread = jnp.where(spread_mask, one, zero).astype(BF16)
    fw = 256
    for f in range(0, hidden, fw):
        cols = slice(f, f + fw)
        g = dot(spread, pre[:, f : f + fw], NN)
        u = dot(spread, pre[:, hidden + f : hidden + f + fw], NN)
        sig = jax.nn.sigmoid(g)
        gs = g * sig
        act_a[:, cols] = gs
        hid[:, cols] = (gs * u).astype(BF16)
        act_b[:, cols] = u * sig * (1.0 + g * (1.0 - sig))

    local[1].wait()

    @pl.loop(1, n_ex)
    def _(k):
        row_copy(sg, rg, dy_s, dy_r, k, ex_from(k), ex_from(k)).wait_recv()

    for i in range(1, n_dp):
        down_copy(i, dp_from(i), dp_peer(i)).wait_recv()
    for f in range(0, hidden, fw):
        cols = slice(f, f + fw)
        hg = dot(rg[...], dfull[:, cols], NN)
        ugrad[:, cols] = (hg * act_a[:, cols]).astype(BF16)
        ggrad[:, cols] = (hg * act_b[:, cols]).astype(BF16)

    def row_grad(n, j):
        out = dot(ggrad[...], gfull[j], NT) + dot(ugrad[...], ufull[j], NT)
        rs[j] = out.astype(BF16)

        @pl.loop(1, n_ex)
        def _(k):
            ret_copy(n, j, k, ex_peer(k), me).start()

        rr[j, block(me), :] = rs[j, block(me), :]

    def combine(n, j):
        @pl.loop(1, n_ex)
        def _(k):
            ret_copy(n, j, k, ex_from(k), ex_from(k)).wait_recv()

        cols = pl.ds(pl.multiple_of(j * cw, cw), cw)
        in_ref[:, cols] = dot(pick, rr[j], NN).astype(BF16)

    for c in range(nc):
        local[3 + 2 * c].wait()
        local[4 + 2 * c].wait()
        row_grad(c, my_dp * nc + c)

    local[2].wait()
    for i in range(1, n_dp):
        base_copy(i, dp_from(i), dp_peer(i)).wait_recv()
    dy_proj = dot(rg[...], bfull[...], NN).astype(BF16)
    terms[2] = dot(dy_proj, hid[...], TN)

    @pl.loop(1, n_ex)
    def _(k):
        row_copy(sx, rx, x_s, x_r, k, ex_from(k), ex_from(k)).wait_recv()

    x_proj = dot(rx[...], bfull[...], NN).astype(BF16)
    terms[0] = dot(x_proj, ggrad[...], TN)
    terms[1] = dot(x_proj, ugrad[...], TN)
    for i in range(1, n_dp):
        theirs = pl.ds(pl.multiple_of(dp_peer(i) * rk, rk), rk)
        psend[i] = terms[:, theirs, :].astype(BF16)
        proj_copy(i, dp_peer(i)).start()

    for c in range(nc):
        combine(c, my_dp * nc + c)

    order = [(i, c) for i in range(1, n_dp) for c in range(nc)]
    for n, (i, c) in enumerate(order):
        gate_copy(i, c, dp_from(i), dp_peer(i)).wait_recv()
        up_copy(i, c, dp_from(i), dp_peer(i)).wait_recv()
        row_grad(nc + n, dp_from(i) * nc + c)
        if n:
            last_i, last_c = order[n - 1]
            combine(nc + n - 1, dp_from(last_i) * nc + last_c)
    last_i, last_c = order[-1]
    combine(nc + len(order) - 1, dp_from(last_i) * nc + last_c)

    mine = pl.ds(pl.multiple_of(my_dp * rk, rk), rk)
    total = terms[:, mine, :]
    for i in range(1, n_dp):
        proj_copy(i, dp_peer(i)).wait_recv()
        total = total + prec[i].astype(F32)
    proj_ref[0] = total

    for i in range(1, n_dp):
        down_copy(i, my_dp, dp_peer(i)).wait_send()
        base_copy(i, my_dp, dp_peer(i)).wait_send()
        proj_copy(i, dp_peer(i)).wait_send()
        for c in range(nc):
            gate_copy(i, c, my_dp, dp_peer(i)).wait_send()
            up_copy(i, c, my_dp, dp_peer(i)).wait_send()

    @pl.loop(1, n_ex)
    def _(k):
        row_copy(sg, rg, dy_s, dy_r, k, ex_peer(k), me).wait_send()
        row_copy(sx, rx, x_s, x_r, k, ex_peer(k), me).wait_send()

    spots = [my_dp * nc + c for c in range(nc)] + [dp_from(i) * nc + c for i, c in order]
    for n, j in enumerate(spots):

        @pl.loop(1, n_ex)
        def _(k, n=n, j=j):
            ret_copy(n, j, k, ex_peer(k), me).wait_send()


def body(
    tokens, out_grad, expert_ids, gate_probs, saved_pre, gate_weight, up_weight, down_weight, basis
):
    n_dp, n_ex = lax.axis_size("dp"), lax.axis_size("expert")
    tok_rows, width = tokens.shape
    slots, hidden2 = saved_pre.shape[2:]
    hidden = hidden2 // 2
    cap = slots // n_ex
    cp = max(16, 1 << (cap - 1).bit_length())
    rows = n_ex * cp
    part = gate_weight.shape[1]
    cw = min(256, part)
    nc = part // cw
    chunks = width // cw
    rank = basis.shape[2]
    rk = rank // n_dp
    vmem = pl.BlockSpec(memory_space=pltpu.VMEM)
    hbm = pl.BlockSpec(memory_space=pl.ANY)
    dma = pltpu.SemaphoreType.DMA
    scratch = [
        pltpu.VMEM((rows, width), BF16),
        pltpu.VMEM((rows, width), BF16),
        pltpu.VMEM((rows, width), BF16),
        pltpu.VMEM((rows, width), BF16),
        pltpu.VMEM((width, hidden), BF16),
        pltpu.VMEM((width, rank), BF16),
        pltpu.VMEM((chunks, cw, hidden), BF16),
        pltpu.VMEM((chunks, cw, hidden), BF16),
        pltpu.VMEM((slots, hidden2), BF16),
        pltpu.VMEM((rows, hidden), F32),
        pltpu.VMEM((rows, hidden), F32),
        pltpu.VMEM((rows, hidden), BF16),
        pltpu.VMEM((rows, hidden), BF16),
        pltpu.VMEM((rows, hidden), BF16),
        pltpu.VMEM((chunks, rows, cw), BF16),
        pltpu.VMEM((chunks, rows, cw), BF16),
        pltpu.VMEM((3, rank, hidden), F32),
        pltpu.VMEM((n_dp, 3, rk, hidden), BF16),
        pltpu.VMEM((n_dp, 3, rk, hidden), BF16),
        dma((3 + 2 * nc,)),
        dma((n_ex,)), dma((n_ex,)), dma((n_ex,)), dma((n_ex,)),
        dma((n_dp,)), dma((n_dp,)), dma((n_dp,)), dma((n_dp,)),
        dma((n_dp, nc)), dma((n_dp, nc)), dma((n_dp, nc)), dma((n_dp, nc)),
        dma((chunks, n_ex)), dma((chunks, n_ex)),
        dma((n_dp,)), dma((n_dp,)),
    ]
    return pl.pallas_call(
        functools.partial(kernel, n_dp, n_ex, cap, cp, cw),
        out_shape=(
            jax.ShapeDtypeStruct((tok_rows, width), BF16),
            jax.ShapeDtypeStruct((1, 3, rk, hidden), F32),
        ),
        in_specs=[vmem] * 4 + [hbm] * 5,
        out_specs=(vmem, vmem),
        scratch_shapes=scratch,
        compiler_params=pltpu.CompilerParams(
            collective_id=0, has_side_effects=True, vmem_limit_bytes=60 * 1024 * 1024
        ),
    )(
        expert_ids, gate_probs, tokens, out_grad, saved_pre,
        gate_weight, up_weight, down_weight, basis,
    )


def solution(mesh):
    return jax.shard_map(
        body,
        mesh=mesh,
        in_specs=(
            P(("dp", "expert"), None),
            P(("dp", "expert"), None),
            P(("dp", "expert"), None),
            P(("dp", "expert"), None),
            P("dp", "expert", None, None),
            P("expert", "dp", None),
            P("expert", "dp", None),
            P("expert", "dp", None),
            P("expert", "dp", None),
        ),
        out_specs=(P(("dp", "expert"), None), P("expert", None, "dp", None)),
        check_vma=False,
    )
```

```python
import functools
import jax
import jax.numpy as jnp
from jax import lax
from jax.experimental import pallas as pl
from jax.experimental.pallas import tpu as pltpu
from jax.sharding import PartitionSpec as P

MESH = pl.DeviceIdType.MESH
F32 = jnp.float32
BF16 = jnp.bfloat16


def dot(left, right, dims):
    return lax.dot_general(left, right, (dims, ((), ())), preferred_element_type=F32)


NN = ((1,), (0,))
TN = ((0,), (0,))
NT = ((1,), (1,))


def kernel(
    n_dp, n_ex, cap, cp, cw,
    ids, probs, tok_h, og_h, pre_h, gw, uw, dw, bs,
    in_ref, own_ref, prec,
    tok, og, sx, sg, rx, rg, dfull, bfull, gfull, ufull, pre, act_a, act_b, hid, ggrad, ugrad,
    rs, rr, terms, psend,
    local_sem, dy_s, dy_r, x_s, x_r, down_s, down_r, base_s, base_r,
    gate_s, gate_r, up_s, up_r, ret_s, ret_r, proj_s, proj_r,
):
    my_dp = lax.axis_index("dp")
    me = lax.axis_index("expert")
    rows = n_ex * cp
    tokens, width = tok.shape
    topk = ids.shape[0]
    slots, hidden2 = pre.shape
    hidden = hidden2 // 2
    part = width // n_dp
    nc = part // cw
    rank = bfull.shape[1]
    rk = rank // n_dp
    shift = cp.bit_length() - 1

    def block(owner):
        return pl.ds(pl.multiple_of(owner * cp, cp), cp)

    def wpart(owner):
        return pl.ds(pl.multiple_of(owner * part, part), part)

    def ex_peer(k):
        return lax.rem(me + k, n_ex)

    def ex_from(k):
        return lax.rem(me + n_ex - k, n_ex)

    def dp_peer(i):
        return lax.rem(my_dp + i, n_dp)

    def dp_from(i):
        return lax.rem(my_dp + n_dp - i, n_dp)

    barrier = pltpu.get_barrier_semaphore()

    @pl.loop(1, n_ex)
    def _(k):
        pl.semaphore_signal(barrier, inc=1, device_id={"expert": ex_peer(k)}, device_id_type=MESH)

    for i in range(1, n_dp):
        pl.semaphore_signal(barrier, inc=1, device_id={"dp": dp_peer(i)}, device_id_type=MESH)

    local = [
        pltpu.make_async_copy(pre_h.at[0, 0], pre, local_sem.at[0]),
        pltpu.make_async_copy(dw.at[0], dfull.at[wpart(my_dp)], local_sem.at[1]),
        pltpu.make_async_copy(bs.at[0], bfull.at[wpart(my_dp)], local_sem.at[2]),
    ]
    local_n = 3 + 2 * nc
    fetch = [
        pltpu.make_async_copy(og_h, og, local_sem.at[local_n]),
        pltpu.make_async_copy(tok_h, tok, local_sem.at[local_n + 1]),
    ]
    for copy in fetch:
        copy.start()
    for c in range(nc):
        src = pl.ds(c * cw, cw)
        local.append(
            pltpu.make_async_copy(gw.at[0, src], gfull.at[my_dp * nc + c], local_sem.at[3 + 2 * c])
        )
        local.append(
            pltpu.make_async_copy(uw.at[0, src], ufull.at[my_dp * nc + c], local_sem.at[4 + 2 * c])
        )
    for copy in local:
        copy.start()

    line = lax.broadcasted_iota(jnp.int32, (rows, tokens), 0)
    line_expert = lax.shift_right_logical(line, shift)
    line_slot = lax.bitwise_and(line, cp - 1)
    names = [ids[k : k + 1, :] == line_expert for k in range(topk)]
    any_name = functools.reduce(jnp.logical_or, names)
    one, zero = jnp.ones((), F32), jnp.zeros((), F32)
    named = jnp.where(any_name, one, zero).astype(BF16)
    earlier = lax.broadcasted_iota(jnp.int32, (tokens, tokens), 0) < lax.broadcasted_iota(
        jnp.int32, (tokens, tokens), 1
    )
    before = dot(named, jnp.where(earlier, one, zero).astype(BF16), NN)
    at_slot = before == line_slot.astype(F32)
    pick = jnp.where(jnp.logical_and(any_name, at_slot), one, zero).astype(BF16)
    weights = functools.reduce(
        jnp.add, [jnp.where(name, probs[k : k + 1, :], zero) for k, name in enumerate(names)]
    )
    weight = jnp.sum(jnp.where(at_slot, weights, zero), axis=1, keepdims=True)
    fetch[0].wait()
    sg[...] = (dot(pick, og[...], NN) * weight).astype(BF16)

    pl.semaphore_wait(barrier, n_ex - 1 + n_dp - 1)

    def down_copy(i, owner, peer):
        return pltpu.make_async_remote_copy(
            dw.at[0], dfull.at[wpart(owner)], down_s.at[i], down_r.at[i],
            device_id={"dp": peer}, device_id_type=MESH,
        )

    def base_copy(i, owner, peer):
        return pltpu.make_async_remote_copy(
            bs.at[0], bfull.at[wpart(owner)], base_s.at[i], base_r.at[i],
            device_id={"dp": peer}, device_id_type=MESH,
        )

    def gate_copy(i, c, owner, peer):
        return pltpu.make_async_remote_copy(
            gw.at[0, pl.ds(c * cw, cw)], gfull.at[owner * nc + c], gate_s.at[i, c], gate_r.at[i, c],
            device_id={"dp": peer}, device_id_type=MESH,
        )

    def up_copy(i, c, owner, peer):
        return pltpu.make_async_remote_copy(
            uw.at[0, pl.ds(c * cw, cw)], ufull.at[owner * nc + c], up_s.at[i, c], up_r.at[i, c],
            device_id={"dp": peer}, device_id_type=MESH,
        )

    def row_copy(src, dst, send, recv, k, peer, owner):
        return pltpu.make_async_remote_copy(
            src.at[block(peer)], dst.at[block(owner)], send.at[k], recv.at[k],
            device_id={"expert": peer}, device_id_type=MESH,
        )

    def ret_copy(n, j, k, peer, owner):
        return pltpu.make_async_remote_copy(
            rs.at[j, block(peer)], rr.at[j, block(owner)], ret_s.at[n, k], ret_r.at[n, k],
            device_id={"expert": peer}, device_id_type=MESH,
        )

    def proj_copy(i, peer):
        return pltpu.make_async_remote_copy(
            psend.at[i - 1], prec.at[i - 1], proj_s.at[i], proj_r.at[i],
            device_id={"dp": peer}, device_id_type=MESH,
        )

    for i in range(1, n_dp):
        down_copy(i, my_dp, dp_peer(i)).start()

    @pl.loop(1, n_ex)
    def _(k):
        row_copy(sg, rg, dy_s, dy_r, k, ex_peer(k), me).start()

    for i in range(1, n_dp):
        base_copy(i, my_dp, dp_peer(i)).start()
    for i in range(1, n_dp):
        for c in range(nc):
            gate_copy(i, c, my_dp, dp_peer(i)).start()
            up_copy(i, c, my_dp, dp_peer(i)).start()

    fetch[1].wait()
    sx[...] = dot(pick, tok[...], NN).astype(BF16)

    @pl.loop(1, n_ex)
    def _(k):
        row_copy(sx, rx, x_s, x_r, k, ex_peer(k), me).start()

    rg[block(me), :] = sg[block(me), :]
    rx[block(me), :] = sx[block(me), :]

    local[0].wait()
    row = lax.broadcasted_iota(jnp.int32, (rows, slots), 0)
    inner = lax.bitwise_and(row, cp - 1)
    source = lax.shift_right_logical(row, shift) * cap + inner
    spread_mask = jnp.logical_and(
        source == lax.broadcasted_iota(jnp.int32, (rows, slots), 1), inner < cap
    )
    spread = jnp.where(spread_mask, one, zero).astype(BF16)
    fw = 256
    for f in range(0, hidden, fw):
        cols = slice(f, f + fw)
        g = dot(spread, pre[:, f : f + fw], NN)
        u = dot(spread, pre[:, hidden + f : hidden + f + fw], NN)
        sig = jax.nn.sigmoid(g)
        gs = g * sig
        act_a[:, cols] = gs
        hid[:, cols] = (gs * u).astype(BF16)
        act_b[:, cols] = u * sig * (1.0 + g * (1.0 - sig))

    local[1].wait()

    @pl.loop(1, n_ex)
    def _(k):
        row_copy(sg, rg, dy_s, dy_r, k, ex_from(k), ex_from(k)).wait_recv()

    for i in range(1, n_dp):
        down_copy(i, dp_from(i), dp_peer(i)).wait_recv()
    for f in range(0, hidden, fw):
        cols = slice(f, f + fw)
        hg = dot(rg[...], dfull[:, cols], NN)
        ugrad[:, cols] = (hg * act_a[:, cols]).astype(BF16)
        ggrad[:, cols] = (hg * act_b[:, cols]).astype(BF16)

    def row_grad(n, j):
        out = dot(ggrad[...], gfull[j], NT) + dot(ugrad[...], ufull[j], NT)
        rs[j] = out.astype(BF16)

        @pl.loop(1, n_ex)
        def _(k):
            ret_copy(n, j, k, ex_peer(k), me).start()

        rr[j, block(me), :] = rs[j, block(me), :]

    def combine(n, j):
        @pl.loop(1, n_ex)
        def _(k):
            ret_copy(n, j, k, ex_from(k), ex_from(k)).wait_recv()

        cols = pl.ds(pl.multiple_of(j * cw, cw), cw)
        in_ref[:, cols] = dot(pick, rr[j], TN).astype(BF16)

    for c in range(nc):
        local[3 + 2 * c].wait()
        local[4 + 2 * c].wait()
        row_grad(c, my_dp * nc + c)

    local[2].wait()
    for i in range(1, n_dp):
        base_copy(i, dp_from(i), dp_peer(i)).wait_recv()
    dy_proj = dot(rg[...], bfull[...], NN).astype(BF16)
    terms[2] = dot(dy_proj, hid[...], TN)

    @pl.loop(1, n_ex)
    def _(k):
        row_copy(sx, rx, x_s, x_r, k, ex_from(k), ex_from(k)).wait_recv()

    x_proj = dot(rx[...], bfull[...], NN).astype(BF16)
    terms[0] = dot(x_proj, ggrad[...], TN)
    terms[1] = dot(x_proj, ugrad[...], TN)
    for i in range(1, n_dp):
        theirs = pl.ds(pl.multiple_of(dp_peer(i) * rk, rk), rk)
        psend[i - 1] = terms[:, theirs, :].astype(BF16)
        proj_copy(i, dp_peer(i)).start()
    mine = pl.ds(pl.multiple_of(my_dp * rk, rk), rk)
    own_copy = pltpu.make_async_copy(
        terms.at[:, mine, :], own_ref, local_sem.at[local_n + 2]
    )
    own_copy.start()

    for c in range(nc):
        combine(c, my_dp * nc + c)

    order = [(i, c) for i in range(1, n_dp) for c in range(nc)]
    for n, (i, c) in enumerate(order):
        gate_copy(i, c, dp_from(i), dp_peer(i)).wait_recv()
        up_copy(i, c, dp_from(i), dp_peer(i)).wait_recv()
        row_grad(nc + n, dp_from(i) * nc + c)
        if n:
            last_i, last_c = order[n - 1]
            combine(nc + n - 1, dp_from(last_i) * nc + last_c)
    last_i, last_c = order[-1]
    combine(nc + len(order) - 1, dp_from(last_i) * nc + last_c)

    own_copy.wait()
    for i in range(1, n_dp):
        proj_copy(i, dp_peer(i)).wait_recv()

    for i in range(1, n_dp):
        down_copy(i, my_dp, dp_peer(i)).wait_send()
        base_copy(i, my_dp, dp_peer(i)).wait_send()
        proj_copy(i, dp_peer(i)).wait_send()
        for c in range(nc):
            gate_copy(i, c, my_dp, dp_peer(i)).wait_send()
            up_copy(i, c, my_dp, dp_peer(i)).wait_send()

    @pl.loop(1, n_ex)
    def _(k):
        row_copy(sg, rg, dy_s, dy_r, k, ex_peer(k), me).wait_send()
        row_copy(sx, rx, x_s, x_r, k, ex_peer(k), me).wait_send()

    spots = [my_dp * nc + c for c in range(nc)] + [dp_from(i) * nc + c for i, c in order]
    for n, j in enumerate(spots):

        @pl.loop(1, n_ex)
        def _(k, n=n, j=j):
            ret_copy(n, j, k, ex_peer(k), me).wait_send()


def finish(n_peers, in_h, own, prec, in_ref, proj_ref, sem):
    copy = pltpu.make_async_copy(in_h, in_ref, sem)
    copy.start()
    total = own[...]
    for i in range(n_peers):
        total = total + prec[i].astype(F32)
    proj_ref[0] = total
    copy.wait()


def body(
    tokens, out_grad, expert_ids, gate_probs, saved_pre, gate_weight, up_weight, down_weight, basis
):
    n_dp, n_ex = lax.axis_size("dp"), lax.axis_size("expert")
    tok_rows, width = tokens.shape
    slots, hidden2 = saved_pre.shape[2:]
    hidden = hidden2 // 2
    cap = slots // n_ex
    cp = max(16, 1 << (cap - 1).bit_length())
    rows = n_ex * cp
    part = gate_weight.shape[1]
    cw = min(256, part)
    nc = part // cw
    chunks = width // cw
    rank = basis.shape[2]
    rk = rank // n_dp
    vmem = pl.BlockSpec(memory_space=pltpu.VMEM)
    hbm = pl.BlockSpec(memory_space=pl.ANY)
    dma = pltpu.SemaphoreType.DMA
    scratch = [
        pltpu.VMEM((tok_rows, width), BF16),
        pltpu.VMEM((tok_rows, width), BF16),
        pltpu.VMEM((rows, width), BF16),
        pltpu.VMEM((rows, width), BF16),
        pltpu.VMEM((rows, width), BF16),
        pltpu.VMEM((rows, width), BF16),
        pltpu.VMEM((width, hidden), BF16),
        pltpu.VMEM((width, rank), BF16),
        pltpu.VMEM((chunks, cw, hidden), BF16),
        pltpu.VMEM((chunks, cw, hidden), BF16),
        pltpu.VMEM((slots, hidden2), BF16),
        pltpu.VMEM((rows, hidden), F32),
        pltpu.VMEM((rows, hidden), F32),
        pltpu.VMEM((rows, hidden), BF16),
        pltpu.VMEM((rows, hidden), BF16),
        pltpu.VMEM((rows, hidden), BF16),
        pltpu.VMEM((chunks, rows, cw), BF16),
        pltpu.VMEM((chunks, rows, cw), BF16),
        pltpu.VMEM((3, rank, hidden), F32),
        pltpu.VMEM((n_dp - 1, 3, rk, hidden), BF16),
        dma((6 + 2 * nc,)),
        dma((n_ex,)), dma((n_ex,)), dma((n_ex,)), dma((n_ex,)),
        dma((n_dp,)), dma((n_dp,)), dma((n_dp,)), dma((n_dp,)),
        dma((n_dp, nc)), dma((n_dp, nc)), dma((n_dp, nc)), dma((n_dp, nc)),
        dma((chunks, n_ex)), dma((chunks, n_ex)),
        dma((n_dp,)), dma((n_dp,)),
    ]
    in_part, own, received = pl.pallas_call(
        functools.partial(kernel, n_dp, n_ex, cap, cp, cw),
        out_shape=(
            jax.ShapeDtypeStruct((tok_rows, width), BF16),
            jax.ShapeDtypeStruct((3, rk, hidden), F32),
            jax.ShapeDtypeStruct((n_dp - 1, 3, rk, hidden), BF16),
        ),
        in_specs=[vmem] * 2 + [hbm] * 7,
        out_specs=(vmem, hbm, hbm),
        scratch_shapes=scratch,
        compiler_params=pltpu.CompilerParams(
            collective_id=0, has_side_effects=True, vmem_limit_bytes=60 * 1024 * 1024
        ),
    )(
        expert_ids.T, gate_probs.T, tokens, out_grad, saved_pre,
        gate_weight, up_weight, down_weight, basis,
    )
    return pl.pallas_call(
        functools.partial(finish, n_dp - 1),
        out_shape=(
            jax.ShapeDtypeStruct((tok_rows, width), BF16),
            jax.ShapeDtypeStruct((1, 3, rk, hidden), F32),
        ),
        in_specs=[hbm, vmem, vmem],
        out_specs=(vmem, vmem),
        scratch_shapes=[dma],
    )(in_part, own, received)


def solution(mesh):
    return jax.shard_map(
        body,
        mesh=mesh,
        in_specs=(
            P(("dp", "expert"), None),
            P(("dp", "expert"), None),
            P(("dp", "expert"), None),
            P(("dp", "expert"), None),
            P("dp", "expert", None, None),
            P("expert", "dp", None),
            P("expert", "dp", None),
            P("expert", "dp", None),
            P("expert", "dp", None),
        ),
        out_specs=(P(("dp", "expert"), None), P("expert", None, "dp", None)),
        check_vma=False,
    )
```

```python
import functools
import jax
import jax.numpy as jnp
from jax import lax
from jax.experimental import pallas as pl
from jax.experimental.pallas import tpu as pltpu
from jax.sharding import PartitionSpec as P

MESH = pl.DeviceIdType.MESH
F32 = jnp.float32
BF16 = jnp.bfloat16


def dot(left, right, dims):
    return lax.dot_general(left, right, (dims, ((), ())), preferred_element_type=F32)


NN = ((1,), (0,))
TN = ((0,), (0,))
NT = ((1,), (1,))


def kernel(
    n_dp, n_ex, cap, cp, cw,
    ids, probs, tok_h, og_h, pre_h, gw, uw, dw, bs,
    in_h, own_ref, prec,
    in_v, tok, og, sx, sg, rx, rg, dfull, bfull, gfull, ufull, pre, act_a, act_b, hid, ggrad, ugrad,
    rs, rr, terms, psend,
    local_sem, dy_s, dy_r, x_s, x_r, down_s, down_r, base_s, base_r,
    gate_s, gate_r, up_s, up_r, ret_s, ret_r, proj_s, proj_r, in_s,
):
    my_dp = lax.axis_index("dp")
    me = lax.axis_index("expert")
    rows = n_ex * cp
    tokens, width = tok.shape
    topk = ids.shape[0]
    slots, hidden2 = pre.shape
    hidden = hidden2 // 2
    part = width // n_dp
    nc = part // cw
    rank = bfull.shape[1]
    rk = rank // n_dp
    shift = cp.bit_length() - 1

    def block(owner):
        return pl.ds(pl.multiple_of(owner * cp, cp), cp)

    def wpart(owner):
        return pl.ds(pl.multiple_of(owner * part, part), part)

    def ex_peer(k):
        return lax.rem(me + k, n_ex)

    def ex_from(k):
        return lax.rem(me + n_ex - k, n_ex)

    def dp_peer(i):
        return lax.rem(my_dp + i, n_dp)

    def dp_from(i):
        return lax.rem(my_dp + n_dp - i, n_dp)

    barrier = pltpu.get_barrier_semaphore()

    @pl.loop(1, n_ex)
    def _(k):
        pl.semaphore_signal(barrier, inc=1, device_id={"expert": ex_peer(k)}, device_id_type=MESH)

    for i in range(1, n_dp):
        pl.semaphore_signal(barrier, inc=1, device_id={"dp": dp_peer(i)}, device_id_type=MESH)

    local = [
        pltpu.make_async_copy(pre_h.at[0, 0], pre, local_sem.at[0]),
        pltpu.make_async_copy(dw.at[0], dfull.at[wpart(my_dp)], local_sem.at[1]),
        pltpu.make_async_copy(bs.at[0], bfull.at[wpart(my_dp)], local_sem.at[2]),
    ]
    local_n = 3 + 2 * nc
    fetch = [
        pltpu.make_async_copy(og_h, og, local_sem.at[local_n]),
        pltpu.make_async_copy(tok_h, tok, local_sem.at[local_n + 1]),
    ]
    for copy in fetch:
        copy.start()
    for c in range(nc):
        src = pl.ds(c * cw, cw)
        local.append(
            pltpu.make_async_copy(gw.at[0, src], gfull.at[my_dp * nc + c], local_sem.at[3 + 2 * c])
        )
        local.append(
            pltpu.make_async_copy(uw.at[0, src], ufull.at[my_dp * nc + c], local_sem.at[4 + 2 * c])
        )
    for copy in local:
        copy.start()

    line = lax.broadcasted_iota(jnp.int32, (rows, tokens), 0)
    line_expert = lax.shift_right_logical(line, shift)
    line_slot = lax.bitwise_and(line, cp - 1)
    names = [ids[k : k + 1, :] == line_expert for k in range(topk)]
    any_name = functools.reduce(jnp.logical_or, names)
    one, zero = jnp.ones((), F32), jnp.zeros((), F32)
    named = jnp.where(any_name, one, zero).astype(BF16)
    earlier = lax.broadcasted_iota(jnp.int32, (tokens, tokens), 0) < lax.broadcasted_iota(
        jnp.int32, (tokens, tokens), 1
    )
    before = dot(named, jnp.where(earlier, one, zero).astype(BF16), NN)
    at_slot = before == line_slot.astype(F32)
    pick = jnp.where(jnp.logical_and(any_name, at_slot), one, zero).astype(BF16)
    weights = functools.reduce(
        jnp.add, [jnp.where(name, probs[k : k + 1, :], zero) for k, name in enumerate(names)]
    )
    weight = jnp.sum(jnp.where(at_slot, weights, zero), axis=1, keepdims=True)
    fetch[0].wait()
    sg[...] = (dot(pick, og[...], NN) * weight).astype(BF16)

    pl.semaphore_wait(barrier, n_ex - 1 + n_dp - 1)

    def down_copy(i, owner, peer):
        return pltpu.make_async_remote_copy(
            dw.at[0], dfull.at[wpart(owner)], down_s.at[i], down_r.at[i],
            device_id={"dp": peer}, device_id_type=MESH,
        )

    def base_copy(i, owner, peer):
        return pltpu.make_async_remote_copy(
            bs.at[0], bfull.at[wpart(owner)], base_s.at[i], base_r.at[i],
            device_id={"dp": peer}, device_id_type=MESH,
        )

    def gate_copy(i, c, owner, peer):
        return pltpu.make_async_remote_copy(
            gw.at[0, pl.ds(c * cw, cw)], gfull.at[owner * nc + c], gate_s.at[i, c], gate_r.at[i, c],
            device_id={"dp": peer}, device_id_type=MESH,
        )

    def up_copy(i, c, owner, peer):
        return pltpu.make_async_remote_copy(
            uw.at[0, pl.ds(c * cw, cw)], ufull.at[owner * nc + c], up_s.at[i, c], up_r.at[i, c],
            device_id={"dp": peer}, device_id_type=MESH,
        )

    def row_copy(src, dst, send, recv, k, peer, owner):
        return pltpu.make_async_remote_copy(
            src.at[block(peer)], dst.at[block(owner)], send.at[k], recv.at[k],
            device_id={"expert": peer}, device_id_type=MESH,
        )

    def ret_copy(n, j, k, peer, owner):
        return pltpu.make_async_remote_copy(
            rs.at[j, block(peer)], rr.at[j, block(owner)], ret_s.at[n, k], ret_r.at[n, k],
            device_id={"expert": peer}, device_id_type=MESH,
        )

    def proj_copy(i, peer):
        return pltpu.make_async_remote_copy(
            psend.at[i - 1], prec.at[i - 1], proj_s.at[i], proj_r.at[i],
            device_id={"dp": peer}, device_id_type=MESH,
        )

    for i in range(1, n_dp):
        down_copy(i, my_dp, dp_peer(i)).start()

    @pl.loop(1, n_ex)
    def _(k):
        row_copy(sg, rg, dy_s, dy_r, k, ex_peer(k), me).start()

    for i in range(1, n_dp):
        base_copy(i, my_dp, dp_peer(i)).start()
    for i in range(1, n_dp):
        for c in range(nc):
            gate_copy(i, c, my_dp, dp_peer(i)).start()
            up_copy(i, c, my_dp, dp_peer(i)).start()

    fetch[1].wait()
    sx[...] = dot(pick, tok[...], NN).astype(BF16)

    @pl.loop(1, n_ex)
    def _(k):
        row_copy(sx, rx, x_s, x_r, k, ex_peer(k), me).start()

    rg[block(me), :] = sg[block(me), :]
    rx[block(me), :] = sx[block(me), :]

    local[0].wait()
    row = lax.broadcasted_iota(jnp.int32, (rows, slots), 0)
    inner = lax.bitwise_and(row, cp - 1)
    source = lax.shift_right_logical(row, shift) * cap + inner
    spread_mask = jnp.logical_and(
        source == lax.broadcasted_iota(jnp.int32, (rows, slots), 1), inner < cap
    )
    spread = jnp.where(spread_mask, one, zero).astype(BF16)
    fw = 256
    for f in range(0, hidden, fw):
        cols = slice(f, f + fw)
        g = dot(spread, pre[:, f : f + fw], NN)
        u = dot(spread, pre[:, hidden + f : hidden + f + fw], NN)
        sig = jax.nn.sigmoid(g)
        gs = g * sig
        act_a[:, cols] = gs
        hid[:, cols] = (gs * u).astype(BF16)
        act_b[:, cols] = u * sig * (1.0 + g * (1.0 - sig))

    local[1].wait()

    @pl.loop(1, n_ex)
    def _(k):
        row_copy(sg, rg, dy_s, dy_r, k, ex_from(k), ex_from(k)).wait_recv()

    for i in range(1, n_dp):
        down_copy(i, dp_from(i), dp_peer(i)).wait_recv()
    for f in range(0, hidden, fw):
        cols = slice(f, f + fw)
        hg = dot(rg[...], dfull[:, cols], NN)
        ugrad[:, cols] = (hg * act_a[:, cols]).astype(BF16)
        ggrad[:, cols] = (hg * act_b[:, cols]).astype(BF16)

    def row_grad(n, j):
        out = dot(ggrad[...], gfull[j], NT) + dot(ugrad[...], ufull[j], NT)
        rs[j] = out.astype(BF16)

        @pl.loop(1, n_ex)
        def _(k):
            ret_copy(n, j, k, ex_peer(k), me).start()

        rr[j, block(me), :] = rs[j, block(me), :]

    stored = []

    def combine(n, j):
        @pl.loop(1, n_ex)
        def _(k):
            ret_copy(n, j, k, ex_from(k), ex_from(k)).wait_recv()

        cols = pl.ds(pl.multiple_of(j * cw, cw), cw)
        in_v[j] = dot(pick, rr[j], TN).astype(BF16)
        stored.append(pltpu.make_async_copy(in_v.at[j], in_h.at[:, cols], in_s.at[n]))
        stored[-1].start()

    for c in range(nc):
        local[3 + 2 * c].wait()
        local[4 + 2 * c].wait()
        row_grad(c, my_dp * nc + c)

    local[2].wait()
    for i in range(1, n_dp):
        base_copy(i, dp_from(i), dp_peer(i)).wait_recv()
    dy_proj = dot(rg[...], bfull[...], NN).astype(BF16)
    terms[2] = dot(dy_proj, hid[...], TN)

    @pl.loop(1, n_ex)
    def _(k):
        row_copy(sx, rx, x_s, x_r, k, ex_from(k), ex_from(k)).wait_recv()

    x_proj = dot(rx[...], bfull[...], NN).astype(BF16)
    terms[0] = dot(x_proj, ggrad[...], TN)
    terms[1] = dot(x_proj, ugrad[...], TN)
    for i in range(1, n_dp):
        theirs = pl.ds(pl.multiple_of(dp_peer(i) * rk, rk), rk)
        psend[i - 1] = terms[:, theirs, :].astype(BF16)
        proj_copy(i, dp_peer(i)).start()
    mine = pl.ds(pl.multiple_of(my_dp * rk, rk), rk)
    own_copy = pltpu.make_async_copy(
        terms.at[:, mine, :], own_ref, local_sem.at[local_n + 2]
    )
    own_copy.start()

    for c in range(nc):
        combine(c, my_dp * nc + c)

    order = [(i, c) for i in range(1, n_dp) for c in range(nc)]
    for n, (i, c) in enumerate(order):
        gate_copy(i, c, dp_from(i), dp_peer(i)).wait_recv()
        up_copy(i, c, dp_from(i), dp_peer(i)).wait_recv()
        row_grad(nc + n, dp_from(i) * nc + c)
        if n:
            last_i, last_c = order[n - 1]
            combine(nc + n - 1, dp_from(last_i) * nc + last_c)
    last_i, last_c = order[-1]
    combine(nc + len(order) - 1, dp_from(last_i) * nc + last_c)

    for i in range(1, n_dp):
        down_copy(i, my_dp, dp_peer(i)).wait_send()
        base_copy(i, my_dp, dp_peer(i)).wait_send()
        for c in range(nc):
            gate_copy(i, c, my_dp, dp_peer(i)).wait_send()
            up_copy(i, c, my_dp, dp_peer(i)).wait_send()

    @pl.loop(1, n_ex)
    def _(k):
        row_copy(sg, rg, dy_s, dy_r, k, ex_peer(k), me).wait_send()
        row_copy(sx, rx, x_s, x_r, k, ex_peer(k), me).wait_send()

    spots = [my_dp * nc + c for c in range(nc)] + [dp_from(i) * nc + c for i, c in order]
    for n, j in enumerate(spots):

        @pl.loop(1, n_ex)
        def _(k, n=n, j=j):
            ret_copy(n, j, k, ex_peer(k), me).wait_send()

    for copy in stored:
        copy.wait()
    own_copy.wait()
    for i in range(1, n_dp):
        proj_copy(i, dp_peer(i)).wait_recv()
        proj_copy(i, dp_peer(i)).wait_send()


def finish(n_peers, in_h, own_h, prec_h, in_ref, proj_ref, rows, own, prec, total, in_s, own_s, prec_s, out_s):
    loads = []
    for t in range(own.shape[0]):
        pieces = [pltpu.make_async_copy(own_h.at[t], own.at[t], own_s.at[t])]
        for i in range(n_peers):
            pieces.append(
                pltpu.make_async_copy(prec_h.at[i, t], prec.at[i, t], prec_s.at[i, t])
            )
        for copy in pieces:
            copy.start()
        loads.append(pieces)
    load = pltpu.make_async_copy(in_h, rows, in_s.at[0])
    load.start()
    stores = []
    for t, pieces in enumerate(loads):
        for copy in pieces:
            copy.wait()
        value = own[t]
        for i in range(n_peers):
            value = value + prec[i, t].astype(F32)
        total[t] = value
        stores.append(pltpu.make_async_copy(total.at[t], proj_ref.at[0, t], out_s.at[t]))
        stores[-1].start()
    load.wait()
    stores.append(pltpu.make_async_copy(rows, in_ref, in_s.at[1]))
    stores[-1].start()
    for copy in stores:
        copy.wait()


def body(
    tokens, out_grad, expert_ids, gate_probs, saved_pre, gate_weight, up_weight, down_weight, basis
):
    n_dp, n_ex = lax.axis_size("dp"), lax.axis_size("expert")
    tok_rows, width = tokens.shape
    slots, hidden2 = saved_pre.shape[2:]
    hidden = hidden2 // 2
    cap = slots // n_ex
    cp = max(16, 1 << (cap - 1).bit_length())
    rows = n_ex * cp
    part = gate_weight.shape[1]
    cw = min(256, part)
    nc = part // cw
    chunks = width // cw
    rank = basis.shape[2]
    rk = rank // n_dp
    vmem = pl.BlockSpec(memory_space=pltpu.VMEM)
    hbm = pl.BlockSpec(memory_space=pl.ANY)
    dma = pltpu.SemaphoreType.DMA
    scratch = [
        pltpu.VMEM((chunks, tok_rows, cw), BF16),
        pltpu.VMEM((tok_rows, width), BF16),
        pltpu.VMEM((tok_rows, width), BF16),
        pltpu.VMEM((rows, width), BF16),
        pltpu.VMEM((rows, width), BF16),
        pltpu.VMEM((rows, width), BF16),
        pltpu.VMEM((rows, width), BF16),
        pltpu.VMEM((width, hidden), BF16),
        pltpu.VMEM((width, rank), BF16),
        pltpu.VMEM((chunks, cw, hidden), BF16),
        pltpu.VMEM((chunks, cw, hidden), BF16),
        pltpu.VMEM((slots, hidden2), BF16),
        pltpu.VMEM((rows, hidden), F32),
        pltpu.VMEM((rows, hidden), F32),
        pltpu.VMEM((rows, hidden), BF16),
        pltpu.VMEM((rows, hidden), BF16),
        pltpu.VMEM((rows, hidden), BF16),
        pltpu.VMEM((chunks, rows, cw), BF16),
        pltpu.VMEM((chunks, rows, cw), BF16),
        pltpu.VMEM((3, rank, hidden), F32),
        pltpu.VMEM((n_dp - 1, 3, rk, hidden), BF16),
        dma((6 + 2 * nc,)),
        dma((n_ex,)), dma((n_ex,)), dma((n_ex,)), dma((n_ex,)),
        dma((n_dp,)), dma((n_dp,)), dma((n_dp,)), dma((n_dp,)),
        dma((n_dp, nc)), dma((n_dp, nc)), dma((n_dp, nc)), dma((n_dp, nc)),
        dma((chunks, n_ex)), dma((chunks, n_ex)),
        dma((n_dp,)), dma((n_dp,)), dma((chunks,)),
    ]
    in_part, own, received = pl.pallas_call(
        functools.partial(kernel, n_dp, n_ex, cap, cp, cw),
        out_shape=(
            jax.ShapeDtypeStruct((tok_rows, width), BF16),
            jax.ShapeDtypeStruct((3, rk, hidden), F32),
            jax.ShapeDtypeStruct((n_dp - 1, 3, rk, hidden), BF16),
        ),
        in_specs=[vmem] * 2 + [hbm] * 7,
        out_specs=(hbm, hbm, hbm),
        scratch_shapes=scratch,
        compiler_params=pltpu.CompilerParams(
            collective_id=0, has_side_effects=True, vmem_limit_bytes=60 * 1024 * 1024
        ),
    )(
        expert_ids.T, gate_probs.T, tokens, out_grad, saved_pre,
        gate_weight, up_weight, down_weight, basis,
    )
    return pl.pallas_call(
        functools.partial(finish, n_dp - 1),
        out_shape=(
            jax.ShapeDtypeStruct((tok_rows, width), BF16),
            jax.ShapeDtypeStruct((1, 3, rk, hidden), F32),
        ),
        in_specs=[hbm, hbm, hbm],
        out_specs=(hbm, hbm),
        scratch_shapes=[
            pltpu.VMEM((tok_rows, width), BF16),
            pltpu.VMEM((3, rk, hidden), F32),
            pltpu.VMEM((n_dp - 1, 3, rk, hidden), BF16),
            pltpu.VMEM((3, rk, hidden), F32),
            dma((2,)), dma((3,)), dma((n_dp - 1, 3)), dma((3,)),
        ],
    )(in_part, own, received)


def solution(mesh):
    return jax.shard_map(
        body,
        mesh=mesh,
        in_specs=(
            P(("dp", "expert"), None),
            P(("dp", "expert"), None),
            P(("dp", "expert"), None),
            P(("dp", "expert"), None),
            P("dp", "expert", None, None),
            P("expert", "dp", None),
            P("expert", "dp", None),
            P("expert", "dp", None),
            P("expert", "dp", None),
        ),
        out_specs=(P(("dp", "expert"), None), P("expert", None, "dp", None)),
        check_vma=False,
    )
```
